32 devices in a mesh: dp: 4 (over y, core), section: 4 (over z), mp: 2 (over x).
Axes of the slice: x: 2, y: 2, z: 4, core: 2. Of those that a mesh axis runs over, the one named last changes fastest.
Arguments:
- feature_bank: bfloat16 [1024, 1152], P('dp'), may hold values from -6 to 6
- feature_scale: float32 [4, 9], P('dp'), may hold values from 0.25 to 4
- shard_owner: int32 [4], replicated, may hold values from 0 to 3, each once
- image_shard: int32 [512, 1], P('dp'), may hold values from 0 to 3; in each aligned block of 128 rows (0 to 127, 128 to 255, ...) at most 64 rows name the same one
- image_row: int32 [512], P('dp'), may hold values from 0 to 255
- text_doc: int32 [4, 1024], P('dp'), may hold values from 0 to 7, never falling along the last dimension, each value on 1 to 512 neighbouring positions
- image_count: int32 [4, 8], P('dp'), may hold values from 1 to 64, 128 in all within a row
- proj_weight: bfloat16 [1152, 8192], P(None, ('section', 'mp')), may hold values from -0.1875 to 0.1875
- kv_weight: bfloat16 [32768, 512], P('section', 'mp'), may hold values from -0.0625 to 0.0625
- queries: bfloat16 [4096, 8192], P('dp', ('section', 'mp')), may hold values from -48 to 48
- out_grad: bfloat16 [4096, 8192], P('dp', ('section', 'mp')), may hold values from -1 to 1
Outputs:
- proj_grad: float32 [1152, 8192], P('dp', ('section', 'mp'))
The draws below stay inside these ranges and needn't reach their ends.
Inputs may be any that keep to these rules, and one draw needn't show every extreme that they name: `image_shard`: the 128 image tokens of one data group name no shard more than 64 times. `shard_owner`: each dp index once. `text_doc`: never falls along a sequence; each of the 8 documents has at least one token. `image_count`: the 8 counts of a data group sum to 128.
All inputs are finite; a program needn't handle non-finite values.
Results may differ from the reference program's by a relative error of at most 0.0085.
Values may be sent and summed in bfloat16 or wider, within the bound.
No kernel may reach another device: no remote copies, remote signals or barrier semaphores. Data moves between devices by JAX's collectives and lax.ppermute only.
A program may use at most 64 MiB of HBM per device.

```python
import math
import jax
import jax.numpy as jnp
import numpy as np
from jax import lax

D = 8192
VIS = 1152
HD = 128
GROUP = 8
QBLK = 128
TOK = 1024
IMG = 128
BANK = 256
DOCS = 8
KVH = 2
QH = 16
NBLK = 9
CAP = 64
TOKENS = 4096
N_DP = 4
N_SECTION = 4


def draw_queries(key, part):
    head_count = N_SECTION * QH
    base_key = jax.random.fold_in(key, 101)
    token_key = jax.random.fold_in(key, 202)
    level_key = jax.random.fold_in(key, 303)
    base_values = jnp.clip(jax.random.normal(base_key, (N_DP, TOK, head_count, HD), jnp.float32), -6.0, 6.0)
    picked_token = jax.random.randint(token_key, (N_DP, head_count), 0, TOK)
    level_index = jax.random.randint(level_key, (N_DP, head_count), 0, 3)
    strength_table = jnp.array([3.0, 4.5, 6.0], jnp.float32)
    strength = jnp.take(strength_table, level_index)
    token_ids = jnp.arange(TOK, dtype=jnp.int32)
    marked = token_ids[None, :, None] == picked_token[:, None, :]
    factor = jnp.where(marked, strength[:, None, :], 1.0)
    boosted = jnp.clip(base_values * factor[:, :, :, None], -48.0, 48.0)
    return boosted.reshape(N_DP * TOK, head_count * HD).astype(jnp.bfloat16)


def plant(entries, own_key, least, top_value):
    dims = entries.shape
    index_at = [jax.random.randint(jax.random.fold_in(own_key, axis), (), 0, dims[axis]) for axis in range(len(dims))]
    entries = entries.at[tuple(index_at)].set(least)
    longest = dims.index(max(dims))
    index_at[longest] = (index_at[longest] + 1) % dims[longest]
    return entries.at[tuple(index_at)].set(top_value)


def shard_levels(key, shape, split, smallest, top_value):
    level, own = 1.0, jax.random.fold_in(key, 6)
    for position, shards_of in split:
        draws = jnp.exp(jax.random.uniform(jax.random.fold_in(own, position), (shards_of,), jnp.float32, smallest / len(split), top_value / len(split)))
        level = level * jnp.repeat(draws, shape[position] // shards_of).reshape([-1 if axis == position else 1 for axis in range(len(shape))])
    return level


def profile(count, total, bound, skew):
    weights = [(1 << 20) // math.isqrt(rank ** skew) + 1 for rank in range(2, count + 1)]
    rest, counts = total - bound - (count - 1), [1] * (count - 1)
    while rest > 0:
        movable = [i for i in range(count - 1) if counts[i] < bound]
        pool, budget = sum([weights[i] for i in movable]), rest
        for i in movable:
            more = min(bound - counts[i], max(1, budget * weights[i] // pool), rest)
            counts[i] = counts[i] + more
            rest = rest - more
    return np.array([bound] + counts)


def uneven(stream_key, count, total, most, skew):
    if count == 2:
        one = jax.random.randint(stream_key, (), max(1, total - most), min(most, total - 1) + 1)
        return jnp.stack([one, total - one])
    tallies = jnp.asarray(profile(count, total, most, skew), jnp.int32)
    pairs = (count - 1) // 2
    giver, taker = tallies[1:1 + 2 * pairs:2], tallies[2:2 + 2 * pairs:2]
    margin = jnp.minimum(giver - 1, most - taker)
    moved = jax.random.randint(jax.random.fold_in(stream_key, 1), (pairs,), 0, 1 << 20) % (margin + 1)
    tallies = tallies.at[1:1 + 2 * pairs:2].set(giver - moved).at[2:2 + 2 * pairs:2].set(taker + moved)
    return tallies[jax.random.permutation(jax.random.fold_in(stream_key, 2), count)]


def shared_out(key, own, number, rows, number_of, top, bound, skew):
    ranking = jax.random.permutation(key, number_of)
    crowded, common = portions_of(number_of, rows * top, bound, skew, True), portions_of(number_of, rows * top, bound, skew, False)
    places = jnp.arange(number_of)

    def named(tallies, turn):
        used = int((tallies > 0).sum())
        fixed = max(1, used // 4)
        passed = fixed + (places - fixed + turn * (used - fixed)) % max(1, number_of - fixed)
        return jnp.zeros((number_of,), jnp.int32).at[ranking[jnp.where(places < fixed, places, passed)]].set(jnp.asarray(tallies, jnp.int32))

    tallies = jnp.where(number % 4 == 0, named(crowded, number // 4), named(common, number - number // 4 - 1))
    mixed = jax.random.permutation(jax.random.fold_in(own, 3), number_of)
    donor, taker = mixed[0:number_of // 2 * 2:2], mixed[1:number_of // 2 * 2:2]
    slack = jnp.minimum(tallies[donor] - 1, bound - tallies[taker]) // 2
    slack = jnp.where((donor == ranking[0]) | (taker == ranking[0]) | (tallies[taker] == 0), 0, jnp.maximum(slack, 0))
    passed = jax.random.randint(jax.random.fold_in(own, 4), (number_of // 2,), 0, 1 << 20) % (slack + 1)
    tallies = tallies.at[donor].add(-passed).at[taker].add(passed)
    members = jnp.searchsorted(jnp.cumsum(tallies), jnp.arange(rows * top), side="right").astype(jnp.int32)
    listing = members.reshape(top, rows).T
    listing = listing[jax.random.permutation(jax.random.fold_in(own, 1), rows)]
    turn = jax.random.randint(jax.random.fold_in(own, 2), (rows, 1), 0, top)
    return jnp.take_along_axis(listing, (jnp.arange(top)[None, :] + turn) % top, axis=1)


def portions_of(count, total, bound, lean, full):
    portions = [(1 << 20) // math.isqrt(standing ** lean) + 1 for standing in range(1, count + 1)]
    largest = bound if full else min(bound, max(-(-total // count), total * portions[0] // sum(portions)))
    least = 1 if total - largest >= count - 1 else 0
    counts, surplus = [largest] + [least] * (count - 1), total - largest - least * (count - 1)
    while surplus > 0:
        candidates = [i for i in range(1, count) if counts[i] < largest] or [i for i in range(1, count) if counts[i] < bound]
        pool, left = sum([portions[i] for i in candidates]), surplus
        for i in candidates:
            addition = min(bound - counts[i], max(1, left * portions[i] // pool), surplus)
            counts[i] = counts[i] + addition
            surplus = surplus - addition
    return np.array(counts)


def noise(stream_key, dims, scale, most, split=(), kind=jnp.bfloat16):
    factor_of = shard_levels(stream_key, dims, split, -0.22, 0.18) if split else 1.0
    values = jax.random.normal(stream_key, dims, jnp.float32) * scale * factor_of
    return jnp.minimum(jnp.maximum(values, -most), most).astype(kind)


def setup_inputs(seed: int = 0) -> dict:
    key_of = jax.random.split(jax.random.key(seed), 12)
    feature_bank = noise(key_of[0], (N_DP * BANK, VIS), 1.0, 6.0, ((0, 4),))
    feature_scale = jnp.clip(jnp.exp(math.log(4.0) - 2.7725887 * jax.random.uniform(key_of[1], (N_DP, NBLK), jnp.float32) ** shard_levels(key_of[1], (N_DP, NBLK), ((0, 4),), -0.2, 0.2)), 0.25, 4.0)
    shard_owner = jax.random.permutation(key_of[2], N_DP).astype(jnp.int32)
    image_shard_keys = jax.random.split(jax.random.fold_in(key_of[3], 1), (N_DP * IMG) // IMG)
    image_shard_turns = jax.random.permutation(jax.random.fold_in(key_of[3], 3), (N_DP * IMG) // IMG)
    image_shard = jax.vmap(lambda own, number: shared_out(jax.random.fold_in(key_of[3], 2), own, number, IMG, N_DP, 1, CAP, 2))(image_shard_keys, image_shard_turns).reshape((N_DP * IMG, 1))
    image_row = plant(jax.random.randint(key_of[4], (N_DP * IMG,), 0, BANK), jax.random.fold_in(key_of[4], 1), 0, BANK - 1).astype(jnp.int32)
    text_doc = jax.vmap(lambda own: jnp.searchsorted(jnp.cumsum(uneven(own, DOCS, TOK, TOK // 2, 1)), jnp.arange(TOK), side="right"))(jax.random.split(key_of[5], N_DP)).reshape((N_DP, TOK)).astype(jnp.int32)
    image_count = jax.vmap(lambda own: uneven(own, DOCS, IMG, IMG // 2, 1))(jax.random.split(key_of[6], N_DP)).reshape((N_DP, DOCS)).astype(jnp.int32)
    proj_weight = noise(key_of[7], (VIS, D), VIS ** -0.5, 0.1875, ((1, 8),))
    kv_weight = noise(key_of[8], (N_SECTION * D, KVH * 2 * HD), D ** -0.5, 0.0625, ((0, 4), (1, 2)))
    queries = draw_queries(jax.random.fold_in(key_of[11], 71), 0)
    out_grad = noise(key_of[10], (TOKENS, N_SECTION * QH * HD), (2.0 / (N_DP * IMG) ** 0.5), 1.0, ((0, 4), (1, 8)))
    return dict(feature_bank=feature_bank, feature_scale=feature_scale, shard_owner=shard_owner, image_shard=image_shard, image_row=image_row, text_doc=text_doc, image_count=image_count, proj_weight=proj_weight, kv_weight=kv_weight, queries=queries, out_grad=out_grad)


def gelu(values):
    inner = 0.7978845608028654 * (values + 0.044715 * values * values * values)
    return 0.5 * values * (1.0 + jnp.tanh(inner))

def gelu_slope(values):
    inner = 0.7978845608028654 * (values + 0.044715 * values * values * values)
    tangent = jnp.tanh(inner)
    return 0.5 * (1.0 + tangent) + 0.5 * values * (1.0 - tangent * tangent) * 0.7978845608028654 * (1.0 + 3.0 * 0.044715 * values * values)

def head_backward(query_heads, grad_heads, key_value, token_doc, image_doc):
    head_size = key_value.shape[-1] // 2
    key_raw = key_value[:, :head_size]
    values_low = key_value[:, head_size:].astype(jnp.bfloat16)
    inv_norm = lax.rsqrt(lax.optimization_barrier(jnp.mean(key_raw * key_raw, axis=-1, keepdims=True)) + 1e-06)
    key_unit = key_raw * inv_norm
    key_low = key_unit.astype(jnp.bfloat16)
    score_scale = head_size ** (-0.5)
    scores = jnp.einsum('tgd,id->gti', query_heads.astype(jnp.float32), key_low.astype(jnp.float32)) * score_scale
    same_doc = (token_doc[:, None] == image_doc[None, :])[None, :, :]
    scores = jnp.where(same_doc, scores, -1e+30)
    row_max = lax.optimization_barrier(jnp.max(scores, axis=-1, keepdims=True))
    raised = jnp.where(same_doc, jnp.exp(scores - row_max), 0.0)
    probs = raised / lax.optimization_barrier(jnp.sum(raised, axis=-1, keepdims=True))
    probs_low = probs.astype(jnp.bfloat16)
    dprobs = jnp.einsum('tgd,id->gti', grad_heads.astype(jnp.float32), values_low.astype(jnp.float32))
    dscores = probs * (dprobs - lax.optimization_barrier(jnp.sum(probs * dprobs, axis=-1, keepdims=True)))
    dscores_low = dscores.astype(jnp.bfloat16)
    dvalues = jnp.einsum('gti,tgd->id', probs_low.astype(jnp.float32), grad_heads.astype(jnp.float32))
    key_grad = jnp.einsum('gti,tgd->id', dscores_low.astype(jnp.float32), query_heads.astype(jnp.float32)) * score_scale
    raw_grad = inv_norm * (key_grad - key_unit * lax.optimization_barrier(jnp.mean(key_grad * key_unit, axis=-1, keepdims=True)))
    return jnp.concatenate([raw_grad, dvalues], axis=-1).astype(jnp.bfloat16)

def group_backward(group_items):
    key_value, query_cols, grad_cols, token_doc, image_doc = group_items
    return jax.vmap(head_backward, in_axes=(1, 1, 1, None, None), out_axes=1)(query_cols, grad_cols, key_value, token_doc, image_doc)

def reference(feature_bank, feature_scale, shard_owner, image_shard, image_row, text_doc, image_count, proj_weight, kv_weight, queries, out_grad):
    owner_dev = shard_owner[image_shard[:, 0]].astype(jnp.int32)
    bank_rows = (owner_dev * BANK + image_row).astype(jnp.int32)
    scale_cols = jnp.repeat(feature_scale, QBLK, axis=1)
    features = (feature_bank[bank_rows].astype(jnp.float32) * scale_cols[owner_dev]).astype(jnp.bfloat16)
    pre_act = jnp.dot(features, proj_weight, preferred_element_type=jnp.float32)
    embedded = gelu(pre_act).astype(jnp.bfloat16)
    doc_ends = jnp.cumsum(image_count, axis=1)
    positions = jnp.arange(IMG, dtype=jnp.int32)
    image_doc = lax.optimization_barrier(jnp.sum((doc_ends[:, None, :] <= positions[None, :, None]).astype(jnp.int32), axis=2)).astype(jnp.int32)
    emb_grad = jnp.zeros((N_DP * IMG, D), jnp.float32)
    width = QH * HD
    for section_index in range(N_SECTION):
        layer_weight = kv_weight[section_index * D:(section_index + 1) * D]
        key_value = jnp.dot(embedded, layer_weight, preferred_element_type=jnp.float32).reshape(N_DP, IMG, KVH, 2 * HD)
        query_cols = queries[:, section_index * width:(section_index + 1) * width].reshape(N_DP, TOK, KVH, GROUP, HD)
        grad_cols = out_grad[:, section_index * width:(section_index + 1) * width].reshape(N_DP, TOK, KVH, GROUP, HD)
        kv_grad = lax.map(group_backward, (key_value, query_cols, grad_cols, text_doc, image_doc))
        emb_grad = emb_grad + jnp.dot(kv_grad.reshape(N_DP * IMG, KVH * 2 * HD), layer_weight.T, preferred_element_type=jnp.float32)
    pre_grad = (emb_grad * gelu_slope(pre_act)).astype(jnp.bfloat16)
    return jnp.dot(features.T, pre_grad, preferred_element_type=jnp.float32)
```

```python
import jax
import jax.numpy as jnp
from jax import lax
from jax.sharding import PartitionSpec as P

QBLK = 128
LAYER_AXES = ("section", "mp")


def gelu(values):
    inner = 0.7978845608028654 * (values + 0.044715 * values * values * values)
    return 0.5 * values * (1.0 + jnp.tanh(inner))


def gelu_slope(values):
    inner = 0.7978845608028654 * (values + 0.044715 * values * values * values)
    tangent = jnp.tanh(inner)
    return 0.5 * (1.0 + tangent) + 0.5 * values * (1.0 - tangent * tangent) * 0.7978845608028654 * (
        1.0 + 3.0 * 0.044715 * values * values
    )


def head_backward(query_heads, grad_heads, key_value, token_doc, image_doc):
    head_size = key_value.shape[-1] // 2
    key_raw = key_value[:, :head_size]
    values_low = key_value[:, head_size:].astype(jnp.bfloat16)
    inv_norm = lax.rsqrt(jnp.mean(key_raw * key_raw, axis=-1, keepdims=True) + 1e-06)
    key_unit = key_raw * inv_norm
    key_low = key_unit.astype(jnp.bfloat16)
    score_scale = head_size ** (-0.5)
    scores = (
        jnp.einsum("tgd,id->gti", query_heads, key_low, preferred_element_type=jnp.float32)
        * score_scale
    )
    same_doc = (token_doc[:, None] == image_doc[None, :])[None, :, :]
    scores = jnp.where(same_doc, scores, -1e30)
    row_max = jnp.max(scores, axis=-1, keepdims=True)
    raised = jnp.where(same_doc, jnp.exp(scores - row_max), 0.0)
    probs = raised / jnp.sum(raised, axis=-1, keepdims=True)
    probs_low = probs.astype(jnp.bfloat16)
    dprobs = jnp.einsum("tgd,id->gti", grad_heads, values_low, preferred_element_type=jnp.float32)
    dscores = probs * (dprobs - jnp.sum(probs * dprobs, axis=-1, keepdims=True))
    dscores_low = dscores.astype(jnp.bfloat16)
    dvalues = jnp.einsum("gti,tgd->id", probs_low, grad_heads, preferred_element_type=jnp.float32)
    key_grad = (
        jnp.einsum("gti,tgd->id", dscores_low, query_heads, preferred_element_type=jnp.float32)
        * score_scale
    )
    raw_grad = inv_norm * (
        key_grad - key_unit * jnp.mean(key_grad * key_unit, axis=-1, keepdims=True)
    )
    return jnp.concatenate([raw_grad, dvalues], axis=-1).astype(jnp.bfloat16)


def ring_order(sections, columns):
    if sections < 2 or columns % 2:
        return list(range(sections * columns))
    cycle = []
    for column in range(columns):
        rows = range(1, sections) if column % 2 == 0 else range(sections - 1, 0, -1)
        cycle += [row * columns + column for row in rows]
    return cycle + [column for column in range(columns - 1, -1, -1)]


def lookup(table, index):
    found = jnp.int32(0)
    for place, value in enumerate(table):
        found = found + jnp.where(index == place, jnp.int32(value), jnp.int32(0))
    return found


class Ring:
    def __init__(self):
        sections, columns = lax.axis_size("section"), lax.axis_size("mp")
        self.order = ring_order(sections, columns)
        self.count = len(self.order)
        place = [0] * self.count
        for position, member in enumerate(self.order):
            place[member] = position
        self.me = lax.axis_index(LAYER_AXES)
        self.position = lookup(place, self.me)

    def member(self, distance):
        return lookup(self.order, (self.position + distance) % self.count)

    def send(self, values, step):
        pairs = [
            (self.order[i], self.order[(i + step) % self.count]) for i in range(self.count)
        ]
        return lax.ppermute(values, LAYER_AXES, pairs)

    def reach(self, piece, step):
        longer, shorter = self.count // 2, (self.count - 1) // 2
        return longer if (piece % 2 == 0) == (step > 0) else shorter


def body(
    feature_bank,
    feature_scale,
    shard_owner,
    image_shard,
    image_row,
    text_doc,
    image_count,
    proj_weight,
    kv_weight,
    queries,
    out_grad,
):
    groups = lax.axis_size("dp")
    images = image_row.shape[0]
    capacity = max(2, 2 * images // groups)
    owner_dev = shard_owner[image_shard[:, 0]]
    chosen = (owner_dev[:, None] == jnp.arange(groups, dtype=jnp.int32)[None, :]).astype(jnp.int32)
    earlier = jnp.cumsum(chosen, axis=0) - chosen
    slot_index = jnp.sum(earlier * chosen, axis=1)
    wanted = (
        jnp.zeros((groups * capacity,), jnp.int32)
        .at[owner_dev * capacity + slot_index]
        .set(image_row)
    )
    wanted = wanted.reshape(groups, capacity)
    columns = jnp.repeat(feature_scale[0], QBLK)
    looked = feature_bank[lax.all_to_all(wanted, "dp", split_axis=0, concat_axis=0, tiled=True)]
    scaled = (looked.astype(jnp.float32) * columns).astype(jnp.bfloat16)
    arrived = lax.all_to_all(scaled, "dp", split_axis=0, concat_axis=0, tiled=True)
    features = arrived[owner_dev, slot_index]

    ring = Ring()
    width = proj_weight.shape[1]
    pieces = 2
    part = width // pieces

    def weight_rows(member, piece):
        return lax.dynamic_slice_in_dim(kv_weight, member * width + piece * part, part, 0)

    def times_weight(values, member, piece):
        return jnp.dot(values, weight_rows(member, piece), preferred_element_type=jnp.float32)

    pre_act = [
        jnp.dot(
            features,
            proj_weight[:, piece * part : (piece + 1) * part],
            preferred_element_type=jnp.float32,
        )
        for piece in range(pieces)
    ]
    own = [gelu(values).astype(jnp.bfloat16) for values in pre_act]
    slope = [gelu_slope(values) for values in pre_act]
    held = {(piece, step): own[piece] for piece in range(pieces) for step in (1, -1)}
    key_value = sum(times_weight(own[piece], ring.me, piece) for piece in range(pieces))
    for hop in range(1, ring.count // 2 + 1):
        for piece in range(pieces):
            for step in (1, -1):
                if hop <= ring.reach(piece, step):
                    held[piece, step] = ring.send(held[piece, step], step)
        for piece in range(pieces):
            for step in (1, -1):
                if hop <= ring.reach(piece, step):
                    key_value = key_value + times_weight(
                        held[piece, step], ring.member(-step * hop), piece
                    )

    doc_ends = jnp.cumsum(image_count[0])
    positions = jnp.arange(images, dtype=jnp.int32)
    image_doc = jnp.sum((doc_ends[None, :] <= positions[:, None]).astype(jnp.int32), axis=1)
    head_size = kv_weight.shape[1] // 2
    tokens = queries.shape[0]
    query_heads = queries.reshape(tokens, -1, head_size)
    grad_heads = out_grad.reshape(tokens, -1, head_size)
    kv_grad = head_backward(query_heads, grad_heads, key_value, text_doc[0], image_doc)

    def share(member, piece):
        return lax.dot_general(
            kv_grad,
            weight_rows(member, piece),
            (((1,), (1,)), ((), ())),
            preferred_element_type=jnp.float32,
        )

    sums = {}
    for hop in range(1, ring.count // 2 + 1):
        for piece in range(pieces):
            for step in (1, -1):
                reach = ring.reach(piece, step)
                if hop <= reach:
                    mine = share(ring.member(step * (reach - hop + 1)), piece)
                    if hop > 1:
                        mine = mine + sums[piece, step].astype(jnp.float32)
                    sums[piece, step] = ring.send(mine.astype(jnp.bfloat16), step)
    rows = features.shape[1] // groups
    me = lax.axis_index("dp")

    def dp_swap(values, mask):
        return lax.ppermute(values, "dp", [(i, i ^ mask) for i in range(groups)])

    if groups == 4:
        feature_parts = [
            lax.dynamic_slice_in_dim(features, (me ^ mask) * rows, rows, 1) for mask in range(groups)
        ]
        feature_parts = [feature_parts[0]] + [
            dp_swap(feature_parts[mask], mask) for mask in range(1, groups)
        ]
    else:
        feature_parts = lax.all_to_all(features, "dp", split_axis=1, concat_axis=0, tiled=True)
    outs = []
    for piece in range(pieces):
        emb_grad = share(ring.me, piece)
        for step in (1, -1):
            emb_grad = emb_grad + sums[piece, step].astype(jnp.float32)
        pre_grad = (emb_grad * slope[piece]).astype(jnp.bfloat16)
        if groups == 4:
            far = dp_swap(pre_grad, 2)
            grads = [pre_grad, dp_swap(pre_grad, 1), far, dp_swap(far, 1)]
            outs.append(
                sum(
                    lax.dot_general(
                        feature_parts[mask],
                        grads[mask],
                        (((0,), (0,)), ((), ())),
                        preferred_element_type=jnp.float32,
                    )
                    for mask in range(groups)
                )
            )
        else:
            outs.append(
                lax.dot_general(
                    feature_parts,
                    lax.all_gather(pre_grad, "dp", axis=0, tiled=True),
                    (((0,), (0,)), ((), ())),
                    preferred_element_type=jnp.float32,
                )
            )
    return jnp.concatenate(outs, axis=1)


def solution(mesh):
    placed = (
        P("dp", None),
        P("dp", None),
        P(),
        P("dp", None),
        P("dp"),
        P("dp", None),
        P("dp", None),
        P(None, ("section", "mp")),
        P("section", "mp"),
        P("dp", ("section", "mp")),
        P("dp", ("section", "mp")),
    )
    return jax.shard_map(
        body, mesh=mesh, in_specs=placed, out_specs=P("dp", ("section", "mp")), check_vma=False
    )
```

```python
import jax
import jax.numpy as jnp
from jax import lax
from jax.experimental import pallas as pl
from jax.experimental.pallas import tpu as pltpu
from jax.sharding import PartitionSpec as P

QBLK = 128
LAYER_AXES = ("section", "mp")
PIECES = 2
SMALL_KERNEL = 4 * 2**20


def gelu(values):
    inner = 0.7978845608028654 * (values + 0.044715 * values * values * values)
    return 0.5 * values * (1.0 + jnp.tanh(inner))


def gelu_slope(values):
    inner = 0.7978845608028654 * (values + 0.044715 * values * values * values)
    tangent = jnp.tanh(inner)
    return 0.5 * (1.0 + tangent) + 0.5 * values * (1.0 - tangent * tangent) * 0.7978845608028654 * (
        1.0 + 3.0 * 0.044715 * values * values
    )


def attention_kernel(count_ref, doc_ref, key_value_ref, query_ref, grad_ref, out_ref):
    head_size = key_value_ref.shape[1] // 2
    images, tokens = key_value_ref.shape[0], query_ref.shape[0]
    heads = query_ref.shape[1] // head_size
    block = min(256, tokens)
    key_raw = key_value_ref[:, :head_size]
    values_low = key_value_ref[:, head_size:].astype(jnp.bfloat16)
    inv_norm = lax.rsqrt(jnp.mean(key_raw * key_raw, axis=-1, keepdims=True) + 1e-06)
    key_unit = key_raw * inv_norm
    key_low = key_unit.astype(jnp.bfloat16)
    score_scale = head_size ** (-0.5)
    exponent_scale = score_scale * 1.4426950408889634
    place = lax.broadcasted_iota(jnp.int32, (images, block), 0)
    image_doc = jnp.zeros((images, block), jnp.int32)
    doc_end = jnp.int32(0)
    for doc in range(count_ref.shape[1]):
        doc_end = doc_end + count_ref[0, doc]
        image_doc = image_doc + (doc_end <= place).astype(jnp.int32)

    together = next(count for count in (4, 2, 1) if heads % count == 0)

    def some_heads(step, sums):
        key_grad, dvalues = sums
        for head in range(together):
            first = (step * together + head) * head_size
            lanes = pl.ds(pl.multiple_of(first, head_size), head_size)
            probs_low, dscores_low = [], []
            for start in range(0, tokens, block):
                scores = lax.dot_general(
                    key_low,
                    query_ref[start : start + block, lanes],
                    (((1,), (1,)), ((), ())),
                    preferred_element_type=jnp.float32,
                )
                dprobs = lax.dot_general(
                    values_low,
                    grad_ref[start : start + block, lanes],
                    (((1,), (1,)), ((), ())),
                    preferred_element_type=jnp.float32,
                )
                same_doc = image_doc == doc_ref[:, start : start + block]
                scores = jnp.where(same_doc, scores * exponent_scale, -1e30)
                raised = jnp.exp2(scores - jnp.max(scores, axis=0, keepdims=True))
                probs = raised * (1.0 / jnp.sum(raised, axis=0, keepdims=True))
                weighted = probs * dprobs
                dscores = weighted - probs * jnp.sum(weighted, axis=0, keepdims=True)
                probs_low.append(probs.astype(jnp.bfloat16))
                dscores_low.append(dscores.astype(jnp.bfloat16))
            dvalues = dvalues + jnp.dot(
                jnp.concatenate(probs_low, axis=1),
                grad_ref[:, lanes],
                preferred_element_type=jnp.float32,
            )
            key_grad = key_grad + jnp.dot(
                jnp.concatenate(dscores_low, axis=1),
                query_ref[:, lanes],
                preferred_element_type=jnp.float32,
            )
        return key_grad, dvalues

    zeros = jnp.zeros((images, head_size), jnp.float32)
    key_grad, dvalues = lax.fori_loop(0, heads // together, some_heads, (zeros, zeros))
    key_grad = key_grad * score_scale
    raw_grad = inv_norm * (
        key_grad - key_unit * jnp.mean(key_grad * key_unit, axis=-1, keepdims=True)
    )
    out_ref[:, :head_size] = raw_grad.astype(jnp.bfloat16)
    out_ref[:, head_size:] = dvalues.astype(jnp.bfloat16)


def attention(image_count, text_doc, key_value, queries, out_grad):
    whole = pl.BlockSpec(memory_space=pltpu.VMEM)
    return pl.pallas_call(
        attention_kernel,
        out_shape=jax.ShapeDtypeStruct(key_value.shape, jnp.bfloat16),
        in_specs=[pl.BlockSpec(memory_space=pltpu.SMEM)] + [whole] * 4,
        out_specs=whole,
        cost_estimate=pl.CostEstimate(
            flops=8 * queries.size * key_value.shape[0],
            bytes_accessed=4 * queries.size,
            transcendentals=queries.size,
        ),
        compiler_params=pltpu.CompilerParams(vmem_limit_bytes=16 * 2**20),
    )(image_count, text_doc, key_value, queries, out_grad)


def slots_of(owner, want, capacity):
    tokens = owner.shape[1]
    chosen = owner == want
    earlier = lax.broadcasted_iota(jnp.int32, (tokens, tokens), 0)
    later = lax.broadcasted_iota(jnp.int32, (tokens, tokens), 1)
    before = jnp.where(earlier < later, 1.0, 0.0).astype(jnp.bfloat16)
    spread = jnp.broadcast_to(jnp.where(chosen, 1.0, 0.0), (16, tokens)).astype(jnp.bfloat16)
    slot = jnp.dot(spread, before, preferred_element_type=jnp.float32)[:1]
    slot = jnp.where(chosen, slot, -1.0)
    place = lax.broadcasted_iota(jnp.int32, (capacity, tokens), 0).astype(jnp.float32)
    return jnp.where(place == slot, 1.0, 0.0).astype(jnp.bfloat16)


def owners(owner_ref, shard):
    owner = jnp.zeros(shard.shape, jnp.int32)
    for index in range(owner_ref.shape[0]):
        owner = jnp.where(shard == index, owner_ref[index], owner)
    return owner


def pick_kernel(owner_ref, me_ref, *refs):
    asked, out_ref = refs[:-1], refs[-1]
    capacity, rows = out_ref.shape[1:]
    for mask, ref in enumerate(asked):
        slots = slots_of(owners(owner_ref, ref[0:1, :]), me_ref[0], capacity)
        row = ref[1:2, :]
        hits = lax.broadcasted_iota(jnp.int32, (rows, row.shape[1]), 0) == row
        out_ref[mask] = lax.dot_general(
            slots,
            jnp.where(hits, 1.0, 0.0).astype(jnp.bfloat16),
            (((1,), (1,)), ((), ())),
            preferred_element_type=jnp.float32,
        ).astype(jnp.bfloat16)


def place_kernel(owner_ref, me_ref, asked_ref, out_ref):
    owner = owners(owner_ref, asked_ref[0:1, :])
    for mask in range(out_ref.shape[0]):
        want = jnp.bitwise_xor(me_ref[0], mask)
        out_ref[mask] = slots_of(owner, want, out_ref.shape[1])


def slot_call(kernel, shape, owner, me, *asked):
    scalar, whole = pl.BlockSpec(memory_space=pltpu.SMEM), pl.BlockSpec(memory_space=pltpu.VMEM)
    return pl.pallas_call(
        kernel,
        out_shape=jax.ShapeDtypeStruct(shape, jnp.bfloat16),
        in_specs=[scalar] * 2 + [whole] * len(asked),
        out_specs=whole,
        cost_estimate=pl.CostEstimate(flops=10**8, bytes_accessed=10**5, transcendentals=0),
        compiler_params=pltpu.CompilerParams(vmem_limit_bytes=SMALL_KERNEL),
    )(owner, me, *asked)


def ring_order(sections, columns):
    if sections < 2 or columns % 2:
        return list(range(sections * columns))
    cycle = []
    for column in range(columns):
        rows = range(1, sections) if column % 2 == 0 else range(sections - 1, 0, -1)
        cycle += [row * columns + column for row in rows]
    return cycle + [column for column in range(columns - 1, -1, -1)]


def lookup(table, index):
    found = jnp.int32(0)
    for place, value in enumerate(table):
        found = found + jnp.where(index == place, jnp.int32(value), jnp.int32(0))
    return found


class Ring:
    def __init__(self):
        sections, columns = lax.axis_size("section"), lax.axis_size("mp")
        self.order = ring_order(sections, columns)
        self.count = len(self.order)
        place = [0] * self.count
        for position, member in enumerate(self.order):
            place[member] = position
        self.me = lax.axis_index(LAYER_AXES)
        self.position = lookup(place, self.me)

    def member(self, distance):
        return lookup(self.order, (self.position + distance) % self.count)

    def pairs(self, step):
        return [(self.order[i], self.order[(i + step) % self.count]) for i in range(self.count)]


def reach(count, piece, step):
    return count // 2 if (piece % 2 == 0) == (step > 0) else (count - 1) // 2


def chains(count, pieces):
    every = [(piece, step) for piece in range(pieces) for step in (1, -1)]
    every.sort(key=lambda chain: -reach(count, *chain))
    return {
        hop: [chain for chain in every if hop <= reach(count, *chain)]
        for hop in range(1, count // 2 + 1)
    }


def body(
    feature_bank,
    feature_scale,
    shard_owner,
    image_shard,
    image_row,
    text_doc,
    image_count,
    proj_weight,
    kv_weight,
    queries,
    out_grad,
):
    groups = lax.axis_size("dp")
    images = image_row.shape[0]
    capacity = max(2, 2 * images // groups)
    columns = jnp.repeat(feature_scale[0], QBLK)
    me = lax.axis_index("dp")

    def dp_swap(values, mask):
        return lax.ppermute(values, "dp", [(i, i ^ mask) for i in range(groups)])

    ring = Ring()
    width = proj_weight.shape[1]
    pieces = PIECES
    part = width // pieces

    def project(values):
        return [
            jnp.dot(
                values,
                proj_weight[:, piece * part : (piece + 1) * part],
                preferred_element_type=jnp.float32,
            )
            for piece in range(pieces)
        ]

    if groups == 4:
        asked = jnp.stack([image_shard[:, 0], image_row])
        others = {mask: dp_swap(asked, mask) for mask in (2, 3, 1)}
        scaled = (feature_bank.astype(jnp.float32) * columns).astype(jnp.bfloat16)
        table = gelu(
            jnp.dot(scaled, proj_weight, preferred_element_type=jnp.float32)
        ).astype(jnp.bfloat16)
        me_ref = me.astype(jnp.int32).reshape(1)
        depth = feature_bank.shape[0]
        places = slot_call(
            place_kernel, (groups, capacity, images), shard_owner, me_ref, asked
        )
        picks = slot_call(
            pick_kernel,
            (groups, capacity, depth),
            shard_owner,
            me_ref,
            asked,
            *(others[mask] for mask in (1, 2, 3)),
        )

        def answers(values):
            arrived = []
            for mask in range(groups):
                rows = jnp.dot(
                    picks[mask], values, preferred_element_type=jnp.float32
                ).astype(jnp.bfloat16)
                arrived.append(dp_swap(rows, mask) if mask else rows)
            return arrived

        def put(arrived):
            total = jnp.float32(0.0)
            for mask, rows in enumerate(arrived):
                total = total + lax.dot_general(
                    places[mask],
                    rows,
                    (((0,), (0,)), ((), ())),
                    preferred_element_type=jnp.float32,
                )
            return total.astype(jnp.bfloat16)

        arrived = answers(table)
        own = [
            put([rows[:, piece * part : (piece + 1) * part] for rows in arrived])
            for piece in range(pieces)
        ]
        features = put(answers(scaled))
        pre_act = project(features)
    else:
        owner_dev = shard_owner[image_shard[:, 0]]
        chosen = (owner_dev[:, None] == jnp.arange(groups, dtype=jnp.int32)[None, :]).astype(
            jnp.int32
        )
        earlier = jnp.cumsum(chosen, axis=0) - chosen
        slot_index = jnp.sum(earlier * chosen, axis=1)
        wanted = (
            jnp.zeros((groups * capacity,), jnp.int32)
            .at[owner_dev * capacity + slot_index]
            .set(image_row)
        )
        wanted = wanted.reshape(groups, capacity)
        looked = feature_bank[lax.all_to_all(wanted, "dp", split_axis=0, concat_axis=0, tiled=True)]
        scaled = (looked.astype(jnp.float32) * columns).astype(jnp.bfloat16)
        arrived = lax.all_to_all(scaled, "dp", split_axis=0, concat_axis=0, tiled=True)
        features = arrived[owner_dev, slot_index]
        pre_act = project(features)
        own = [gelu(values).astype(jnp.bfloat16) for values in pre_act]
    slope = [gelu_slope(values) for values in pre_act]

    def weight_rows(member, piece):
        return lax.dynamic_slice_in_dim(kv_weight, member * width + piece * part, part, 0)

    def times_weight(values, member, piece):
        return jnp.dot(values, weight_rows(member, piece), preferred_element_type=jnp.float32)

    held = {(piece, step): own[piece] for piece in range(pieces) for step in (1, -1)}
    key_value = sum(times_weight(own[piece], ring.me, piece) for piece in range(pieces))
    for hop, members in chains(ring.count, pieces).items():
        for piece, step in members:
            held[piece, step] = lax.ppermute(held[piece, step], LAYER_AXES, ring.pairs(step))
            key_value = key_value + times_weight(held[piece, step], ring.member(-step * hop), piece)

    kv_grad = attention(image_count, text_doc, key_value, queries, out_grad)

    def share(member, piece):
        return lax.dot_general(
            kv_grad,
            weight_rows(member, piece),
            (((1,), (1,)), ((), ())),
            preferred_element_type=jnp.float32,
        )

    sums = {}
    for hop, members in chains(ring.count, pieces).items():
        for piece, step in members:
            most = reach(ring.count, piece, step)
            mine = share(ring.member(step * (most - hop + 1)), piece)
            if hop > 1:
                mine = mine + sums[piece, step].astype(jnp.float32)
            mine = mine.astype(jnp.bfloat16)
            sums[piece, step] = lax.ppermute(mine, LAYER_AXES, ring.pairs(step))
    rows = features.shape[1] // groups
    if groups == 4:
        feature_parts = [
            lax.dynamic_slice_in_dim(features, (me ^ mask) * rows, rows, 1)
            for mask in range(groups)
        ]
        feature_parts = [feature_parts[0]] + [
            dp_swap(feature_parts[mask], mask) for mask in range(1, groups)
        ]
    pre_grad = []
    for piece in range(pieces):
        emb_grad = share(ring.me, piece)
        for step in (1, -1):
            emb_grad = emb_grad + sums[piece, step].astype(jnp.float32)
        pre_grad.append((emb_grad * slope[piece]).astype(jnp.bfloat16))

    def transposed_dot(left, right):
        return lax.dot_general(
            left, right, (((0,), (0,)), ((), ())), preferred_element_type=jnp.float32
        )

    if groups != 4:
        grads = [lax.all_gather(values, "dp", axis=0, tiled=True) for values in pre_grad]
        parts = lax.all_to_all(features, "dp", split_axis=1, concat_axis=0, tiled=True)
        return transposed_dot(parts, jnp.concatenate(grads, axis=1))
    far = jnp.concatenate([dp_swap(values, 2) for values in pre_grad], axis=1)
    near = jnp.concatenate(pre_grad, axis=1)
    grads = [near, dp_swap(near, 1), far, dp_swap(far, 1)]
    out = sum(transposed_dot(feature_parts[mask], grads[mask]) for mask in range(groups - 1))
    return lax.optimization_barrier(out) + transposed_dot(feature_parts[-1], grads[-1])


def solution(mesh):
    placed = (
        P("dp", None),
        P("dp", None),
        P(),
        P("dp", None),
        P("dp"),
        P("dp", None),
        P("dp", None),
        P(None, ("section", "mp")),
        P("section", "mp"),
        P("dp", ("section", "mp")),
        P("dp", ("section", "mp")),
    )

    return jax.shard_map(
        body, mesh=mesh, in_specs=placed, out_specs=P("dp", ("section", "mp")), check_vma=False
    )
```
